32 devices in a mesh: group: 2 (over x), seq: 16 (over z, y, core).
Axes of the slice: x: 2, y: 2, z: 4, core: 2. Of those that a mesh axis runs over, the one named last changes fastest.
Arguments:
- tokens: bfloat16 [16384, 4096], P(('group', 'seq')), parts along dimension 0, may hold values from -6 to 6
- norm_gain: bfloat16 [4096], replicated, may hold values from 0.099609375 to 1.8984375
- w_key: bfloat16 [4096, 1024], P('seq'), may hold values from -0.09375 to 0.09375
- w_value: bfloat16 [4096, 1024], P('seq'), may hold values from -0.09375 to 0.09375
- lengths: int32 [4], P('group'), parts along dimension 0, may hold values from 2048 to 4096
- page_table: int32 [1024], P(('group', 'seq')), parts along dimension 0, may hold values from 0 to 639, as said below
Outputs:
- kv_cache: bfloat16 [2, 1280, 16, 1024], P(None, ('group', 'seq')), parts along dimension 1
The draws below stay inside these ranges and needn't reach their ends.
There are 2 independent parts, one for each index of `group`. The reference program is written for one: setup_inputs(seed, part) draws one part's arguments, and reference() takes and returns one part's arrays. A program takes and returns all parts, laid end to end along the dimension named above; an argument that names none is the same for every part. Nothing has to cross between parts.
Inputs may be any that keep to these rules, and one draw needn't show every extreme that they name: The entries are distinct. Page g of the 32 pages of device s goes to slot page_table[g] of decode device page_table[g] // 40, which is s + k modulo 16 for an offset k in -2 .. 2, at a slot of the block of 8 slots from (k + 2) * 8 on; so at most 8 pages go from one device to one decode device, and exactly 8 from every device to some decode device.
All inputs are finite; a program needn't handle non-finite values.
Results may differ from the reference program's by a relative error of at most 0.0049.
Values may be sent and summed in bfloat16 or wider, within the bound.
A program may use at most 64 MiB of HBM per device.

```python
import jax
import jax.numpy as jnp
from jax import lax

D = 4096
HEAD = 128
PAGE = 16
REACH = 2
TOK_DEV = 512
KVD = 1024
TOKENS = 8192
LENGTH = 4096
CAP = 8
SLOTS = 40
PAGES = 512
N_SEQ = 16


def draw_page_table(key, part):
    pages_dev = TOK_DEV // PAGE
    regions = 2 * REACH + 1

    def one_device(device):
        device_key = jax.random.fold_in(jax.random.fold_in(key, 7), device)
        first_key, second_key, third_key = jax.random.split(device_key, 3)
        full_region = jax.random.randint(first_key, (), 0, regions)
        ranks = jax.random.permutation(second_key, SLOTS)
        region_of = jnp.arange(SLOTS, dtype=jnp.int32) // CAP
        score = jnp.where(region_of == full_region, 0, SLOTS) + ranks
        order = jnp.argsort(score, stable=True)
        chosen = jax.random.permutation(third_key, order[:pages_dev])
        offset = chosen // CAP - REACH
        target = (device + offset) % N_SEQ
        return (target * SLOTS + chosen).astype(jnp.int32)
    table = jax.vmap(one_device)(jnp.arange(N_SEQ, dtype=jnp.int32))
    return table.reshape(-1).astype(jnp.int32)


def block_levels(key, shape, shards, low, top_value):
    factor_of = 1.0
    for axis_at, parts in shards:
        heights = jax.random.uniform(jax.random.fold_in(jax.random.fold_in(key, 6), axis_at), (parts,), jnp.float32, low / len(shards), top_value / len(shards))
        factor_of = factor_of * jnp.repeat(jnp.exp(heights), shape[axis_at] // parts).reshape((-1,) + (1,) * (len(shape) - 1 - axis_at))
    return factor_of


def bell_draw(own_key, extent, spread, most, cuts=(), kind=jnp.bfloat16):
    values = jax.random.normal(own_key, extent, jnp.float32) * spread
    if len(cuts) > 0:
        values = block_levels(own_key, extent, cuts, -0.22, 0.18) * values
    return jnp.clip(values, min=-most, max=most).astype(kind)


def setup_inputs(seed: int = 0, part: int = 0) -> dict:
    key_list = jax.random.split(jax.random.key(seed), 7)
    part_splits = jax.random.split(jax.random.fold_in(key_list[6], part), 7)
    return {
        "tokens": bell_draw(part_splits[0], (TOKENS, D), 1.0, 6.0, ((0, 16),)),
        "norm_gain": jnp.clip(1.0 + 0.18 * jax.random.normal(key_list[1], (D,), jnp.float32), 0.099609375, 1.8984375).astype(jnp.bfloat16),
        "w_key": bell_draw(key_list[2], (D, KVD), D ** -0.5, 0.09375, ((0, 16),)),
        "w_value": bell_draw(key_list[3], (D, KVD), D ** -0.5, 0.09375, ((0, 16),)),
        "lengths": jax.random.randint(part_splits[4], (2,), LENGTH // 2, LENGTH + 1).astype(jnp.int32),
        "page_table": draw_page_table(jax.random.fold_in(jax.random.fold_in(key_list[6], part), 71), part),
    }


ROPE_THETA = 500000.0
EPS = 1e-05

def rotate_keys(key_rows, position):
    half = HEAD // 2
    freq = ROPE_THETA ** (-(jnp.arange(half, dtype=jnp.float32) * 2.0 / HEAD))
    angle = position.astype(jnp.float32)[:, None] * freq[None, :]
    cosine = jnp.cos(angle)[:, None, :]
    sine = jnp.sin(angle)[:, None, :]
    shaped = key_rows.reshape(key_rows.shape[0], -1, HEAD)
    first = shaped[:, :, :half]
    second = shaped[:, :, half:]
    turned = jnp.concatenate([first * cosine - second * sine, second * cosine + first * sine], axis=2)
    return turned.reshape(key_rows.shape)

def reference(tokens, norm_gain, w_key, w_value, lengths, page_table):
    wide = tokens.astype(jnp.float32)
    scale = lax.rsqrt(lax.optimization_barrier(jnp.mean(wide * wide, axis=1, keepdims=True)) + EPS)
    normed = (wide * scale * norm_gain.astype(jnp.float32)[None, :]).astype(jnp.bfloat16)
    key_rows = jnp.dot(normed, w_key, preferred_element_type=jnp.float32)
    value_rows = jnp.dot(normed, w_value, preferred_element_type=jnp.float32)
    token_index = jnp.arange(TOKENS, dtype=jnp.int32)
    prompt_id = token_index // LENGTH
    position = token_index % LENGTH
    limit = jnp.where(prompt_id == 0, lengths[0], lengths[1])
    inside = (position < limit)[:, None]
    key_rows = rotate_keys(key_rows, position)
    keys = jnp.where(inside, key_rows, 0.0).astype(jnp.bfloat16)
    values = jnp.where(inside, value_rows, 0.0).astype(jnp.bfloat16)
    pages = jnp.stack([keys, values]).reshape(2, PAGES, PAGE, KVD)
    cache = jnp.zeros((2, N_SEQ * SLOTS, PAGE, KVD), jnp.bfloat16)
    return cache.at[:, page_table.astype(jnp.int32)].set(pages)
```

```python
import functools

import jax
import jax.numpy as jnp
from jax import lax
from jax.experimental import pallas as pl
from jax.experimental.pallas import tpu as pltpu
from jax.sharding import PartitionSpec as P

HEAD = 128
PAGE = 16
REACH = 2
CAP = 8
SLOTS = 40
REGIONS = 2 * REACH + 1
BLOCK = CAP * PAGE
ROWS = SLOTS * PAGE

ROPE_THETA = 500000.0
EPS = 1e-05

CHUNKS = 4
TILE = 256
MESH = pl.DeviceIdType.MESH


def kernel(
    n, tokens, gain, w_key, w_value, dest, cosine, sine, out,
    wbuf, xbuf, pbuf, onehot,
    load_sem, tok_sem, zs, zr, ys, yr, xs, xr, ds, dr, cs, cr, hs, hr,
):
    chunks, depth = wbuf.shape[0], wbuf.shape[1]
    half, width = wbuf.shape[5], wbuf.shape[6]
    per_kind = chunks // 2
    tok_rows, features = xbuf.shape
    group = lax.axis_index("group")
    me = lax.axis_index("seq")
    core, y, z = lax.rem(me, 2), lax.rem(me // 2, 2), me // 4
    other_core, other_y, other_group = 1 - core, 1 - y, 1 - group

    def seq_of(z_at, y_at, core_at):
        return (z_at * 2 + y_at) * 2 + core_at

    def piece(j, z_at, y_at, part):
        return wbuf.at[j, z_at, y_at, core, part]

    def send(ref, send_sem, recv_sem, group_at, seq_at, dst=None):
        pltpu.make_async_remote_copy(
            src_ref=ref,
            dst_ref=ref if dst is None else dst,
            send_sem=send_sem,
            recv_sem=recv_sem,
            device_id={"group": group_at, "seq": seq_at},
            device_id_type=MESH,
        ).start()

    def wait(ref, sem):
        pltpu.make_async_copy(ref, ref, sem).wait()

    loads = []
    for j in range(chunks):
        w_ref = w_key if j < per_kind else w_value
        columns = pl.ds((j % per_kind) * width, width)
        for part in range(2):
            copy = pltpu.make_async_copy(
                w_ref.at[pl.ds(part * half, half), columns],
                wbuf.at[j, z, y, core, part],
                load_sem.at[j, part],
            )
            copy.start()
            loads.append(copy)
    token_copy = pltpu.make_async_copy(tokens, xbuf, tok_sem)
    token_copy.start()

    to_y = seq_of(z, other_y, core)
    to_core = seq_of(z, y, other_core)

    barrier = pltpu.get_barrier_semaphore()

    def greet(group_at, seq_at):
        pl.semaphore_signal(
            barrier, inc=1, device_id={"group": group_at, "seq": seq_at}, device_id_type=MESH
        )

    def greet_z(k, carry):
        greet(group, seq_of(lax.rem(z + k, depth), y, core))
        return carry

    lax.fori_loop(1, depth, greet_z, 0)
    greet(group, to_y)
    greet(group, to_core)
    greet(other_group, me)
    for region in range(REGIONS):
        if region != REACH:
            greet(group, lax.rem(me + region - REACH + n, n))
    pl.semaphore_wait(barrier, depth - 1 + 3 + REGIONS - 1)

    for copy in loads:
        copy.wait()

    def along_z(j):
        def body(k, carry):
            send(piece(j, z, y, group), zs.at[j], zr.at[j, z], group,
                 seq_of(lax.rem(z + k, depth), y, core))
            return carry

        lax.fori_loop(1, depth, body, 0)

    def to_partner(j, ref):
        send(ref, cs.at[j], cr.at[j], group, to_core)

    def spread(j):
        own = piece(j, z, y, group)
        send(own, ys.at[j], yr.at[j, z], group, to_y)
        to_partner(j, own)
        to_partner(j, piece(j, z, y, other_group))

        def body(k, carry):
            zz = lax.rem(z + k, depth)
            ref = piece(j, zz, y, group)
            wait(ref, zr.at[j, zz])
            send(ref, ys.at[j], yr.at[j, zz], group, to_y)
            send(ref, xs.at[j], xr.at[j, zz], other_group, me)
            to_partner(j, ref)
            return carry

        lax.fori_loop(1, depth, body, 0)

    def relay(j):
        def body(k, carry):
            zz = lax.rem(z + k, depth)
            ref = piece(j, zz, other_y, group)
            wait(ref, yr.at[j, zz])
            send(ref, ds.at[j], dr.at[j, zz], other_group, me)
            to_partner(j, ref)

            @pl.when(k > 0)
            def _():
                crossed = piece(j, zz, y, other_group)
                wait(crossed, xr.at[j, zz])
                to_partner(j, crossed)

            return carry

        lax.fori_loop(0, depth, body, 0)

    def finish(j):
        def body(k, carry):
            zz = lax.rem(z + k, depth)
            ref = piece(j, zz, other_y, other_group)
            wait(ref, dr.at[j, zz])
            to_partner(j, ref)
            return carry

        lax.fori_loop(0, depth, body, 0)
        wait(wbuf.at[j, :, :, other_core], cr.at[j])

    def normalise():
        token_copy.wait()

        def body(i, carry):
            rows = pl.ds(pl.multiple_of(i * 32, 32), 32)
            wide = xbuf[rows, :].astype(jnp.float32)
            scale = lax.rsqrt(jnp.mean(wide * wide, axis=1, keepdims=True) + EPS)
            xbuf[rows, :] = (wide * scale * gain[...]).astype(jnp.bfloat16)
            return carry

        lax.fori_loop(0, tok_rows // 32, body, 0)

        def hot(i, carry):
            rows = lax.broadcasted_iota(jnp.int32, (BLOCK, tok_rows), 0) + i * BLOCK
            onehot[pl.ds(pl.multiple_of(i * BLOCK, BLOCK), BLOCK), :] = jnp.where(
                rows == dest[...], 1.0, 0.0
            ).astype(jnp.bfloat16)
            return carry

        lax.fori_loop(0, REGIONS, hot, 0)

    def project(j):
        def body(t, carry):
            at = pl.multiple_of(t * TILE, TILE)
            weights = wbuf[j, :, :, :, :, :, pl.ds(at, TILE)].reshape(features, TILE)
            raw = jnp.dot(xbuf[...], weights, preferred_element_type=jnp.float32)
            if j < per_kind:
                heads = []
                for head in range(TILE // HEAD):
                    one = raw[:, head * HEAD : (head + 1) * HEAD]
                    heads.append(
                        one * cosine[...] + pltpu.roll(one, HEAD // 2, 1) * sine[...]
                    )
                raw = jnp.concatenate(heads, axis=1)
            placed = jnp.dot(
                onehot[...], raw.astype(jnp.bfloat16), preferred_element_type=jnp.float32
            )
            pbuf[j, :, pl.ds(at, TILE)] = placed.astype(jnp.bfloat16)
            return carry

        lax.fori_loop(0, width // TILE, body, 0)

    def spot(j, region):
        rows = pl.ds(region * BLOCK, BLOCK)
        return (
            pbuf.at[j, rows, :],
            out.at[j // per_kind, rows, pl.ds((j % per_kind) * width, width)],
        )

    def hand_over(j):
        for region in (0, 4, 1, 3, 2):
            src, dst = spot(j, region)
            if region == REACH:
                pltpu.make_async_copy(src, dst, hr.at[j, region]).start()
            else:
                send(src, hs.at[j, region], hr.at[j, region], group,
                     lax.rem(me + region - REACH + n, n), dst)

    for j in range(chunks):
        along_z(j)
    spread(0)
    normalise()
    spread(1)
    relay(0)
    for j in range(chunks):
        if j + 2 < chunks:
            spread(j + 2)
        if j + 1 < chunks:
            relay(j + 1)
        finish(j)
        project(j)
        hand_over(j)

    for j in range(chunks):
        wait(wbuf.at[j, 1:, y, core, group], zs.at[j])
        wait(wbuf.at[j, :, y, core, group], ys.at[j])
        wait(wbuf.at[j, 1:, y, core, group], xs.at[j])
        wait(wbuf.at[j, :, other_y, core, group], ds.at[j])
        wait(wbuf.at[j, :, :, core], cs.at[j])
        for region in range(REGIONS):
            src, dst = spot(j, region)
            wait(dst, hr.at[j, region])
            if region != REACH:
                wait(src, hs.at[j, region])


def on_device(n, tokens, norm_gain, w_key, w_value, lengths, page_table):
    device_index = lax.axis_index("seq")
    tok_rows, features = tokens.shape
    columns = w_key.shape[1]
    length_each = tok_rows * n // 2
    token_index = device_index * tok_rows + jnp.arange(tok_rows, dtype=jnp.int32)
    position = token_index % length_each
    limit = jnp.where(token_index // length_each == 0, lengths[0], lengths[1])
    row = (page_table % SLOTS)[:, None] * PAGE + jnp.arange(PAGE, dtype=jnp.int32)[None, :]
    dest = jnp.where(position < limit, row.reshape(tok_rows), -1)[None, :]
    half_head = HEAD // 2
    freq = ROPE_THETA ** (-(jnp.arange(half_head, dtype=jnp.float32) * 2.0 / HEAD))
    angle = position.astype(jnp.float32)[:, None] * freq[None, :]
    angle = jnp.concatenate([angle, angle], axis=1)
    sign = jnp.where(jnp.arange(HEAD) < half_head, -1.0, 1.0).astype(jnp.float32)
    cosine = jnp.cos(angle)
    sine = jnp.sin(angle) * sign[None, :]
    gain = norm_gain.astype(jnp.float32)[None, :]
    depth = n // 4
    half = w_key.shape[0] // 2
    width = 2 * columns // CHUNKS
    dma = pltpu.SemaphoreType.DMA
    vmem = pl.BlockSpec(memory_space=pltpu.VMEM)
    hbm = pl.BlockSpec(memory_space=pl.ANY)
    cache = pl.pallas_call(
        functools.partial(kernel, n),
        out_shape=jax.ShapeDtypeStruct((2, ROWS, columns), jnp.bfloat16),
        in_specs=[hbm, vmem, hbm, hbm, vmem, vmem, vmem],
        out_specs=hbm,
        scratch_shapes=[
            pltpu.VMEM((CHUNKS, depth, 2, 2, 2, half, width), jnp.bfloat16),
            pltpu.VMEM((tok_rows, features), jnp.bfloat16),
            pltpu.VMEM((CHUNKS, ROWS, width), jnp.bfloat16),
            pltpu.VMEM((ROWS, tok_rows), jnp.bfloat16),
            dma((CHUNKS, 2)),
            dma,
            dma((CHUNKS,)), dma((CHUNKS, depth)),
            dma((CHUNKS,)), dma((CHUNKS, depth)),
            dma((CHUNKS,)), dma((CHUNKS, depth)),
            dma((CHUNKS,)), dma((CHUNKS, depth)),
            dma((CHUNKS,)), dma((CHUNKS,)),
            dma((CHUNKS, REGIONS)), dma((CHUNKS, REGIONS)),
        ],
        compiler_params=pltpu.CompilerParams(
            collective_id=0, has_side_effects=True, vmem_limit_bytes=60 * 2**20
        ),
    )(tokens, gain, w_key, w_value, dest, cosine, sine)
    return cache.reshape(2, SLOTS, PAGE, columns)


def solution(mesh):
    placed = (
        P(("group", "seq"), None),
        P(),
        P("seq", None),
        P("seq", None),
        P("group"),
        P(("group", "seq")),
    )
    return jax.shard_map(
        functools.partial(on_device, mesh.shape["seq"]),
        mesh=mesh,
        in_specs=placed,
        out_specs=P(None, ("group", "seq"), None, None),
        check_vma=False,
    )
```

```python
import functools

import jax
import jax.numpy as jnp
from jax import lax
from jax.experimental import pallas as pl
from jax.experimental.pallas import tpu as pltpu
from jax.sharding import PartitionSpec as P

HEAD = 128
PAGE = 16
REACH = 2
CAP = 8
SLOTS = 40
REGIONS = 2 * REACH + 1
BLOCK = CAP * PAGE
ROWS = SLOTS * PAGE

ROPE_THETA = 500000.0
EPS = 1e-05

CHUNKS = 8
TILE = 256
WAVE = 8
MESH = pl.DeviceIdType.MESH


def kernel(
    n, tokens, gain, w_key, w_value, lengths, pages, freq, out,
    wbuf, xbuf, pbuf, onehot, cosine, sine,
    load_sem, tok_sem, ys, yr, zs, zr, xs, xr, cs, cr, hs, hr,
):
    chunks, depth = wbuf.shape[0], wbuf.shape[1]
    half, width = wbuf.shape[5], wbuf.shape[6]
    per_kind = chunks // 2
    tok_rows, features = xbuf.shape
    group = lax.axis_index("group")
    me = lax.axis_index("seq")
    core, y, z = lax.rem(me, 2), lax.rem(me // 2, 2), me // 4
    other_core, other_y, other_group = 1 - core, 1 - y, 1 - group

    def seq_of(z_at, y_at, core_at):
        return (z_at * 2 + y_at) * 2 + core_at

    def piece(j, z_at, y_at, part):
        return wbuf.at[j, z_at, y_at, core, part]

    def send(ref, send_sem, recv_sem, group_at, seq_at, dst=None):
        pltpu.make_async_remote_copy(
            src_ref=ref,
            dst_ref=ref if dst is None else dst,
            send_sem=send_sem,
            recv_sem=recv_sem,
            device_id={"group": group_at, "seq": seq_at},
            device_id_type=MESH,
        ).start()

    def wait(ref, sem):
        pltpu.make_async_copy(ref, ref, sem).wait()

    loads = []
    for j in range(chunks):
        w_ref = w_key if j < per_kind else w_value
        columns = pl.ds((j % per_kind) * width, width)
        for part in range(2):
            copy = pltpu.make_async_copy(
                w_ref.at[pl.ds(part * half, half), columns],
                wbuf.at[j, z, y, core, part],
                load_sem.at[j, part],
            )
            copy.start()
            loads.append(copy)
    token_copy = pltpu.make_async_copy(tokens, xbuf, tok_sem)
    token_copy.start()

    to_y = seq_of(z, other_y, core)
    to_core = seq_of(z, y, other_core)
    has_up, has_down = z + 1 < depth, z > 0
    up = seq_of(lax.rem(z + 1, depth), y, core)
    down = seq_of(lax.rem(z + depth - 1, depth), y, core)

    barrier = pltpu.get_barrier_semaphore()

    def greet(group_at, seq_at):
        pl.semaphore_signal(
            barrier, inc=1, device_id={"group": group_at, "seq": seq_at}, device_id_type=MESH
        )

    greet(group, up)
    greet(group, down)
    greet(group, to_y)
    greet(group, to_core)
    greet(other_group, me)
    for region in range(REGIONS):
        if region != REACH:
            greet(group, lax.rem(me + region - REACH + n, n))
    pl.semaphore_wait(barrier, 5 + REGIONS - 1)

    def to_partner(j, ref):
        send(ref, cs.at[j], cr.at[j], group, to_core)

    def go_up(j, z_at, y_at, k):
        @pl.when(has_up)
        def _():
            send(piece(j, z_at, y_at, group), zs.at[j, 0, k], zr.at[j, y_at, z_at], group, up)

    def go_down(j, z_at, y_at, k):
        @pl.when(has_down)
        def _():
            send(piece(j, z_at, y_at, group), zs.at[j, 1, k], zr.at[j, y_at, z_at], group, down)

    def begin(j):
        for part in (0, 1):
            ref = piece(j, z, y, part)
            send(ref, ys.at[j], yr.at[j, part], group, to_y)
        go_up(j, z, y, 0)
        go_down(j, z, y, 0)
        for part in (0, 1):
            to_partner(j, piece(j, z, y, part))

    def cross(j):
        for part in (0, 1):
            wait(piece(j, z, other_y, part), yr.at[j, part])
        go_up(j, z, other_y, 0)
        go_down(j, z, other_y, 0)
        for part in (0, 1):
            to_partner(j, piece(j, z, other_y, part))

    def arrive(j, z_at, y_at):
        ref = piece(j, z_at, y_at, group)
        wait(ref, zr.at[j, y_at, z_at])
        return ref

    def pass_on(j, ref, z_at, y_at):
        send(ref, xs.at[j], xr.at[j, y_at, z_at], other_group, me)
        to_partner(j, ref)

    def along(j, k):
        for y_at in (y, other_y):
            @pl.when(z - k >= 0)
            def _():
                ref = arrive(j, z - k, y_at)
                go_up(j, z - k, y_at, k)
                pass_on(j, ref, z - k, y_at)

            @pl.when(z + k < depth)
            def _():
                ref = arrive(j, z + k, y_at)
                go_down(j, z + k, y_at, k)
                pass_on(j, ref, z + k, y_at)

    def finish(j):
        def body(k, carry):
            for y_at in (y, other_y):
                @pl.when(z - k >= 0)
                def _():
                    ref = piece(j, z - k, y_at, other_group)
                    wait(ref, xr.at[j, y_at, z - k])
                    to_partner(j, ref)

                @pl.when(z + k < depth)
                def _():
                    ref = piece(j, z + k, y_at, other_group)
                    wait(ref, xr.at[j, y_at, z + k])
                    to_partner(j, ref)

            return carry

        lax.fori_loop(1, depth, body, 0)

    def prepare():
        token_copy.wait()
        length_each = tok_rows * n // 2

        def body(i, carry):
            rows = pl.ds(pl.multiple_of(i * 32, 32), 32)
            wide = xbuf[rows, :].astype(jnp.float32)
            scale = lax.rsqrt(jnp.mean(wide * wide, axis=1, keepdims=True) + EPS)
            xbuf[rows, :] = (wide * scale * gain[...].astype(jnp.float32)).astype(jnp.bfloat16)
            return carry

        lax.fori_loop(0, tok_rows // 32, body, 0)

        first = lax.rem(me * tok_rows, length_each)
        second_prompt = (me * tok_rows) // length_each
        limit = lengths[0] + second_prompt * (lengths[1] - lengths[0])
        page_count = tok_rows // PAGE
        token = lax.broadcasted_iota(jnp.int32, (page_count, tok_rows), 1)
        page = lax.broadcasted_iota(jnp.int32, (page_count, tok_rows), 0)
        used = jnp.where((token // PAGE == page) & (first + token < limit), 1.0, 0.0)
        used = used.astype(jnp.bfloat16)
        slot = lax.rem(pages[...], SLOTS)

        def hot(i, carry):
            at = i * BLOCK
            row = lax.broadcasted_iota(jnp.int32, (BLOCK, page_count), 0) + at
            held = jnp.where(row // PAGE == slot, 1.0, 0.0).astype(jnp.bfloat16)
            spread = jnp.dot(held, used, preferred_element_type=jnp.float32)
            row = lax.broadcasted_iota(jnp.int32, (BLOCK, tok_rows), 0)
            column = lax.broadcasted_iota(jnp.int32, (BLOCK, tok_rows), 1)
            same = lax.rem(row, PAGE) == lax.rem(column, PAGE)
            onehot[pl.ds(pl.multiple_of(at, BLOCK), BLOCK), :] = jnp.where(
                same, spread, 0.0
            ).astype(jnp.bfloat16)
            return carry

        lax.fori_loop(0, REGIONS, hot, 0)

        def turn(i, carry):
            at = pl.multiple_of(i * 64, 64)
            row = lax.broadcasted_iota(jnp.int32, (64, HEAD), 0) + (first + at)
            lane = lax.broadcasted_iota(jnp.int32, (64, HEAD), 1)
            angle = row.astype(jnp.float32) * freq[...]
            cosine[pl.ds(at, 64), :] = jnp.cos(angle)
            sined = jnp.sin(angle)
            sine[pl.ds(at, 64), :] = jnp.where(lane < HEAD // 2, -sined, sined)
            return carry

        lax.fori_loop(0, tok_rows // 64, turn, 0)

    def project(j):
        wait(wbuf.at[j, :, :, other_core], cr.at[j])
        for t in range(width // TILE):
            at = t * TILE
            weights = wbuf[j, :, :, :, :, :, at : at + TILE].reshape(features, TILE)
            raw = jnp.dot(xbuf[...], weights, preferred_element_type=jnp.float32)
            if j < per_kind:
                heads = []
                for head in range(TILE // HEAD):
                    one = raw[:, head * HEAD : (head + 1) * HEAD]
                    heads.append(
                        one * cosine[...] + pltpu.roll(one, HEAD // 2, 1) * sine[...]
                    )
                raw = jnp.concatenate(heads, axis=1)
            placed = jnp.dot(
                onehot[...], raw.astype(jnp.bfloat16), preferred_element_type=jnp.float32
            )
            pbuf[j, :, at : at + TILE] = placed.astype(jnp.bfloat16)

    def spot(j, region):
        rows = pl.ds(region * BLOCK, BLOCK)
        return (
            pbuf.at[j, rows, :],
            out.at[j // per_kind, rows, pl.ds((j % per_kind) * width, width)],
        )

    def hand_over(j):
        for region in (0, 4, 1, 3, 2):
            src, dst = spot(j, region)
            if region == REACH:
                pltpu.make_async_copy(src, dst, hr.at[j, region]).start()
            else:
                send(src, hs.at[j, region], hr.at[j, region], group,
                     lax.rem(me + region - REACH + n, n), dst)

    def stage(j, k):
        if k == 0:
            cross(j)
        else:
            along(j, k)

    for j in range(chunks):
        for copy in loads[2 * j : 2 * j + 2]:
            copy.wait()
        begin(j)
    if depth <= WAVE:
        for t in range(chunks + depth + 1):
            for j in range(chunks):
                k = t - j
                if 0 <= k < depth:
                    stage(j, k)
            if t == 1:
                prepare()
            if 0 <= t - depth < chunks:
                finish(t - depth)
            if 0 <= t - depth - 1 < chunks:
                project(t - depth - 1)
                hand_over(t - depth - 1)
    else:
        prepare()
        for j in range(chunks):
            stage(j, 0)
            lax.fori_loop(1, depth, lambda k, carry: (along(j, k), carry)[1], 0)
            finish(j)
            project(j)
            hand_over(j)

    for j in range(chunks):
        wait(wbuf.at[j, z, y, core], ys.at[j])
        wait(wbuf.at[j, 1:, :, core, group], xs.at[j])
        wait(wbuf.at[j, :, :, core], cs.at[j])

        def drain(k, carry):
            @pl.when(has_up & (z - k >= 0))
            def _():
                wait(wbuf.at[j, 0, :, core, group], zs.at[j, 0, k])

            @pl.when(has_down & (z + k < depth))
            def _():
                wait(wbuf.at[j, 0, :, core, group], zs.at[j, 1, k])

            return carry

        lax.fori_loop(0, depth, drain, 0)
        for region in range(REGIONS):
            src, dst = spot(j, region)
            wait(dst, hr.at[j, region])
            if region != REACH:
                wait(src, hs.at[j, region])


def on_device(n, tokens, norm_gain, w_key, w_value, lengths, page_table):
    tok_rows, features = tokens.shape
    columns = w_key.shape[1]
    freq = ROPE_THETA ** (-(jnp.arange(HEAD // 2, dtype=jnp.float32) * 2.0 / HEAD))
    freq = jnp.concatenate([freq, freq])[None, :]
    depth = n // 4
    half = w_key.shape[0] // 2
    width = 2 * columns // CHUNKS
    dma = pltpu.SemaphoreType.DMA
    vmem = pl.BlockSpec(memory_space=pltpu.VMEM)
    smem = pl.BlockSpec(memory_space=pltpu.SMEM)
    hbm = pl.BlockSpec(memory_space=pl.ANY)
    cache = pl.pallas_call(
        functools.partial(kernel, n),
        out_shape=jax.ShapeDtypeStruct((2, ROWS, columns), jnp.bfloat16),
        in_specs=[hbm, vmem, hbm, hbm, smem, vmem, vmem],
        out_specs=hbm,
        scratch_shapes=[
            pltpu.VMEM((CHUNKS, depth, 2, 2, 2, half, width), jnp.bfloat16),
            pltpu.VMEM((tok_rows, features), jnp.bfloat16),
            pltpu.VMEM((CHUNKS, ROWS, width), jnp.bfloat16),
            pltpu.VMEM((ROWS, tok_rows), jnp.bfloat16),
            pltpu.VMEM((tok_rows, HEAD), jnp.float32),
            pltpu.VMEM((tok_rows, HEAD), jnp.float32),
            dma((CHUNKS, 2)),
            dma,
            dma((CHUNKS,)), dma((CHUNKS, 2)),
            dma((CHUNKS, 2, depth)), dma((CHUNKS, 2, depth)),
            dma((CHUNKS,)), dma((CHUNKS, 2, depth)),
            dma((CHUNKS,)), dma((CHUNKS,)),
            dma((CHUNKS, REGIONS)), dma((CHUNKS, REGIONS)),
        ],
        compiler_params=pltpu.CompilerParams(
            collective_id=0, has_side_effects=True, vmem_limit_bytes=60 * 2**20
        ),
    )(tokens, norm_gain[None, :], w_key, w_value, lengths, page_table[None, :], freq)
    return cache.reshape(2, SLOTS, PAGE, columns)


def solution(mesh):
    placed = (
        P(("group", "seq"), None),
        P(),
        P("seq", None),
        P("seq", None),
        P("group"),
        P(("group", "seq")),
    )
    return jax.shard_map(
        functools.partial(on_device, mesh.shape["seq"]),
        mesh=mesh,
        in_specs=placed,
        out_specs=P(None, ("group", "seq"), None, None),
        check_vma=False,
    )
```

```python
import functools

import jax
import jax.numpy as jnp
import numpy as np
from jax import lax
from jax.experimental import pallas as pl
from jax.experimental.pallas import tpu as pltpu
from jax.sharding import PartitionSpec as P

HEAD = 128
PAGE = 16
REACH = 2
CAP = 8
SLOTS = 40
REGIONS = 2 * REACH + 1
BLOCK = CAP * PAGE
ROWS = SLOTS * PAGE

ROPE_THETA = 500000.0
EPS = 1e-05

CHUNKS = 8
TILE = 256
WAVE = 8
LAG = 2
MIXED = (0, 2, 4)
MESH = pl.DeviceIdType.MESH


def kernel(
    n, tokens, gain, w_key, w_value, lengths, pages, freq, out,
    wbuf, xbuf, pbuf, onehot, cosine, sine,
    load_sem, tok_sem, ys, yr, fr, zs, zr, xs, xr, cs, cr, hs, hr,
):
    chunks, depth = wbuf.shape[0], wbuf.shape[1]
    half, width = wbuf.shape[5], wbuf.shape[6]
    per_kind = chunks // 2
    tok_rows, features = xbuf.shape
    group = lax.axis_index("group")
    me = lax.axis_index("seq")
    core, y, z = lax.rem(me, 2), lax.rem(me // 2, 2), me // 4
    other_core, other_y, other_group = 1 - core, 1 - y, 1 - group

    def seq_of(z_at, y_at, core_at):
        return (z_at * 2 + y_at) * 2 + core_at

    def piece(j, z_at, y_at, part):
        return wbuf.at[j, z_at, y_at, core, part]

    def send(ref, send_sem, recv_sem, group_at, seq_at, dst=None):
        pltpu.make_async_remote_copy(
            src_ref=ref,
            dst_ref=ref if dst is None else dst,
            send_sem=send_sem,
            recv_sem=recv_sem,
            device_id={"group": group_at, "seq": seq_at},
            device_id_type=MESH,
        ).start()

    def wait(ref, sem):
        pltpu.make_async_copy(ref, ref, sem).wait()

    loads = []
    for j in range(chunks):
        w_ref = w_key if j < per_kind else w_value
        columns = pl.ds((j % per_kind) * width, width)
        for part in range(2):
            copy = pltpu.make_async_copy(
                w_ref.at[pl.ds(part * half, half), columns],
                wbuf.at[j, z, y, core, part],
                load_sem.at[j, part],
            )
            copy.start()
            loads.append(copy)
    token_copy = pltpu.make_async_copy(tokens, xbuf, tok_sem)
    token_copy.start()

    to_y = seq_of(z, other_y, core)
    to_core = seq_of(z, y, other_core)
    has_up, has_down = z + 1 < depth, z > 0
    up = seq_of(lax.rem(z + 1, depth), y, core)
    down = seq_of(lax.rem(z + depth - 1, depth), y, core)

    barrier = pltpu.get_barrier_semaphore()

    def greet(group_at, seq_at):
        pl.semaphore_signal(
            barrier, inc=1, device_id={"group": group_at, "seq": seq_at}, device_id_type=MESH
        )

    greet(group, up)
    greet(group, down)
    greet(group, to_y)
    greet(group, to_core)
    greet(other_group, me)
    for region in range(REGIONS):
        if region != REACH:
            greet(group, lax.rem(me + region - REACH + n, n))
    pl.semaphore_wait(barrier, 5 + REGIONS - 1)

    def to_partner(j, ref):
        send(ref, cs.at[j], cr.at[j], group, to_core)

    def go_up(j, z_at, y_at, k):
        @pl.when(has_up)
        def _():
            send(piece(j, z_at, y_at, group), zs.at[j, 0, k], zr.at[j, y_at, z_at], group, up)

    def go_down(j, z_at, y_at, k):
        @pl.when(has_down)
        def _():
            send(piece(j, z_at, y_at, group), zs.at[j, 1, k], zr.at[j, y_at, z_at], group, down)

    def begin(j):
        for part in (0, 1):
            ref = piece(j, z, y, part)
            send(ref, ys.at[j], yr.at[j, part], group, to_y)
        go_up(j, z, y, 0)
        go_down(j, z, y, 0)
        for part in (0, 1):
            to_partner(j, piece(j, z, y, part))

    def cross(j):
        for part in (0, 1):
            wait(piece(j, z, other_y, part), yr.at[j, part])
        if j not in MIXED:
            go_up(j, z, other_y, 0)
            go_down(j, z, other_y, 0)
        for part in (0, 1):
            to_partner(j, piece(j, z, other_y, part))

    def arrive(j, z_at, y_at):
        ref = piece(j, z_at, y_at, group)
        wait(ref, zr.at[j, y_at, z_at])
        return ref

    def pass_on(j, ref, z_at, y_at):
        send(ref, xs.at[j], xr.at[j, y_at, z_at], other_group, me)
        to_partner(j, ref)
        if j in MIXED:
            send(ref, ys.at[j], fr.at[j, 0, z_at], group, to_y)

    def lines(j):
        return (y,) if j in MIXED else (y, other_y)

    def along(j, k):
        for y_at in lines(j):
            @pl.when(z - k >= 0)
            def _():
                ref = arrive(j, z - k, y_at)
                go_up(j, z - k, y_at, k)
                pass_on(j, ref, z - k, y_at)

            @pl.when(z + k < depth)
            def _():
                ref = arrive(j, z + k, y_at)
                go_down(j, z + k, y_at, k)
                pass_on(j, ref, z + k, y_at)

    def others(visit):
        def body(k, carry):
            @pl.when(z - k >= 0)
            def _():
                visit(z - k)

            @pl.when(z + k < depth)
            def _():
                visit(z + k)

            return carry

        lax.fori_loop(1, depth, body, 0)

    def finish(j):
        def visit(zz):
            for y_at in lines(j):
                ref = piece(j, zz, y_at, other_group)
                wait(ref, xr.at[j, y_at, zz])
                if j in MIXED:
                    send(ref, ys.at[j], fr.at[j, 1, zz], group, to_y)
                to_partner(j, ref)
            if j in MIXED:
                ref = piece(j, zz, other_y, group)
                wait(ref, fr.at[j, 0, zz])
                to_partner(j, ref)

        others(visit)

    def settle(j):
        def visit(zz):
            ref = piece(j, zz, other_y, other_group)
            wait(ref, fr.at[j, 1, zz])
            to_partner(j, ref)

        if j in MIXED:
            others(visit)

    length_each = tok_rows * n // 2
    first = lax.rem(me * tok_rows, length_each)

    def normalise(at, rows_here):
        def body(i, carry):
            rows = pl.ds(pl.multiple_of(at + i * 32, 32), 32)
            wide = xbuf[rows, :].astype(jnp.float32)
            scale = lax.rsqrt(jnp.mean(wide * wide, axis=1, keepdims=True) + EPS)
            xbuf[rows, :] = (wide * scale * gain[...].astype(jnp.float32)).astype(jnp.bfloat16)
            return carry

        lax.fori_loop(0, rows_here // 32, body, 0)

    def mark_rows():
        second_prompt = (me * tok_rows) // length_each
        limit = lengths[0] + second_prompt * (lengths[1] - lengths[0])
        page_count = tok_rows // PAGE
        token = lax.broadcasted_iota(jnp.int32, (page_count, tok_rows), 1)
        page = lax.broadcasted_iota(jnp.int32, (page_count, tok_rows), 0)
        used = jnp.where((token // PAGE == page) & (first + token < limit), 1.0, 0.0)
        used = used.astype(jnp.bfloat16)
        slot = lax.rem(pages[...], SLOTS)

        def hot(i, carry):
            at = i * BLOCK
            row = lax.broadcasted_iota(jnp.int32, (BLOCK, page_count), 0) + at
            held = jnp.where(row // PAGE == slot, 1.0, 0.0).astype(jnp.bfloat16)
            spread = jnp.dot(held, used, preferred_element_type=jnp.float32)
            row = lax.broadcasted_iota(jnp.int32, (BLOCK, tok_rows), 0)
            column = lax.broadcasted_iota(jnp.int32, (BLOCK, tok_rows), 1)
            same = lax.rem(row, PAGE) == lax.rem(column, PAGE)
            onehot[pl.ds(pl.multiple_of(at, BLOCK), BLOCK), :] = jnp.where(
                same, spread, 0.0
            ).astype(jnp.bfloat16)
            return carry

        lax.fori_loop(0, REGIONS, hot, 0)

    def angles():
        def turn(i, carry):
            at = pl.multiple_of(i * 64, 64)
            row = lax.broadcasted_iota(jnp.int32, (64, HEAD), 0) + (first + at)
            lane = lax.broadcasted_iota(jnp.int32, (64, HEAD), 1)
            angle = row.astype(jnp.float32) * freq[...]
            cosine[pl.ds(at, 64), :] = jnp.cos(angle)
            sined = jnp.sin(angle)
            sine[pl.ds(at, 64), :] = jnp.where(lane < HEAD // 2, -sined, sined)
            return carry

        lax.fori_loop(0, tok_rows // 64, turn, 0)

    def project(j):
        wait(wbuf.at[j, :, :, other_core], cr.at[j])
        for t in range(width // TILE):
            at = t * TILE
            weights = wbuf[j, :, :, :, :, :, at : at + TILE].reshape(features, TILE)
            raw = jnp.dot(xbuf[...], weights, preferred_element_type=jnp.float32)
            if j < per_kind:
                heads = []
                for head in range(TILE // HEAD):
                    one = raw[:, head * HEAD : (head + 1) * HEAD]
                    heads.append(
                        one * cosine[...] + pltpu.roll(one, HEAD // 2, 1) * sine[...]
                    )
                raw = jnp.concatenate(heads, axis=1)
            placed = jnp.dot(
                onehot[...], raw.astype(jnp.bfloat16), preferred_element_type=jnp.float32
            )
            pbuf[j, :, at : at + TILE] = placed.astype(jnp.bfloat16)

    def spot(j, region):
        rows = pl.ds(region * BLOCK, BLOCK)
        return (
            pbuf.at[j, rows, :],
            out.at[j // per_kind, rows, pl.ds((j % per_kind) * width, width)],
        )

    def hand_over(j):
        for region in (0, 4, 1, 3, 2):
            src, dst = spot(j, region)
            if region == REACH:
                pltpu.make_async_copy(src, dst, hr.at[j, region]).start()
            else:
                send(src, hs.at[j, region], hr.at[j, region], group,
                     lax.rem(me + region - REACH + n, n), dst)

    def stage(j, k):
        if k == 0:
            cross(j)
        else:
            along(j, k)

    for j in range(chunks):
        for copy in loads[2 * j : 2 * j + 2]:
            copy.wait()
        begin(j)
    quarter = tok_rows // 4
    jobs = [token_copy.wait]
    jobs += [functools.partial(normalise, i * quarter, quarter) for i in range(4)]
    jobs += [mark_rows, angles]
    if depth <= WAVE:
        for t in range(chunks + depth + LAG):
            for j in range(chunks):
                k = t - j
                if 0 <= k < depth:
                    stage(j, k)
            for job in jobs[2 * t : 2 * t + 2]:
                job()
            if 0 <= t - depth < chunks:
                finish(t - depth)
            if 0 <= t - depth - 1 < chunks:
                settle(t - depth - 1)
            if 0 <= t - depth - LAG < chunks:
                project(t - depth - LAG)
                hand_over(t - depth - LAG)
    else:
        for job in jobs:
            job()
        for j in range(chunks):
            stage(j, 0)
            lax.fori_loop(1, depth, lambda k, carry: (along(j, k), carry)[1], 0)
            finish(j)
            settle(j)
            project(j)
            hand_over(j)

    for j in range(chunks):
        if j in MIXED:
            wait(wbuf.at[j, :, y, core], ys.at[j])
            wait(wbuf.at[j, 1:, y, core, group], xs.at[j])
        else:
            wait(wbuf.at[j, z, y, core], ys.at[j])
            wait(wbuf.at[j, 1:, :, core, group], xs.at[j])
        sent = wbuf.at[j, 0, :, core, group]
        if j in MIXED:
            sent = wbuf.at[j, 0, y, core, group]
        wait(wbuf.at[j, :, :, core], cs.at[j])

        def drain(k, carry):
            @pl.when(has_up & (z - k >= 0))
            def _():
                wait(sent, zs.at[j, 0, k])

            @pl.when(has_down & (z + k < depth))
            def _():
                wait(sent, zs.at[j, 1, k])

            return carry

        lax.fori_loop(0, depth, drain, 0)
        for region in range(REGIONS):
            src, dst = spot(j, region)
            wait(dst, hr.at[j, region])
            if region != REACH:
                wait(src, hs.at[j, region])


def on_device(n, tokens, norm_gain, w_key, w_value, lengths, page_table):
    tok_rows, features = tokens.shape
    columns = w_key.shape[1]
    freq = ROPE_THETA ** (-(np.arange(HEAD // 2) * 2.0 / HEAD))
    freq = np.concatenate([freq, freq]).astype(np.float32)[None, :]
    depth = n // 4
    half = w_key.shape[0] // 2
    width = 2 * columns // CHUNKS
    dma = pltpu.SemaphoreType.DMA
    vmem = pl.BlockSpec(memory_space=pltpu.VMEM)
    smem = pl.BlockSpec(memory_space=pltpu.SMEM)
    hbm = pl.BlockSpec(memory_space=pl.ANY)
    cache = pl.pallas_call(
        functools.partial(kernel, n),
        out_shape=jax.ShapeDtypeStruct((2, ROWS, columns), jnp.bfloat16),
        in_specs=[hbm, vmem, hbm, hbm, smem, vmem, vmem],
        out_specs=hbm,
        scratch_shapes=[
            pltpu.VMEM((CHUNKS, depth, 2, 2, 2, half, width), jnp.bfloat16),
            pltpu.VMEM((tok_rows, features), jnp.bfloat16),
            pltpu.VMEM((CHUNKS, ROWS, width), jnp.bfloat16),
            pltpu.VMEM((ROWS, tok_rows), jnp.bfloat16),
            pltpu.VMEM((tok_rows, HEAD), jnp.float32),
            pltpu.VMEM((tok_rows, HEAD), jnp.float32),
            dma((CHUNKS, 2)),
            dma,
            dma((CHUNKS,)), dma((CHUNKS, 2)), dma((CHUNKS, 2, depth)),
            dma((CHUNKS, 2, depth)), dma((CHUNKS, 2, depth)),
            dma((CHUNKS,)), dma((CHUNKS, 2, depth)),
            dma((CHUNKS,)), dma((CHUNKS,)),
            dma((CHUNKS, REGIONS)), dma((CHUNKS, REGIONS)),
        ],
        compiler_params=pltpu.CompilerParams(
            collective_id=0, has_side_effects=True, vmem_limit_bytes=60 * 2**20
        ),
    )(tokens, norm_gain[None, :], w_key, w_value, lengths, page_table[None, :], freq)
    return cache.reshape(2, SLOTS, PAGE, columns)


def solution(mesh):
    placed = (
        P(("group", "seq"), None),
        P(),
        P("seq", None),
        P("seq", None),
        P("group"),
        P(("group", "seq")),
    )
    return jax.shard_map(
        functools.partial(on_device, mesh.shape["seq"]),
        mesh=mesh,
        in_specs=placed,
        out_specs=P(None, ("group", "seq"), None, None),
        check_vma=False,
    )
```
